32 devices in a mesh: group: 4 (over y, core), dev: 8 (over z, x).
Axes of the slice: x: 2, y: 2, z: 4, core: 2. Of those that a mesh axis runs over, the one named last changes fastest.
Arguments:
- points: bfloat16 [8192, 256], P(('group', 'dev')), may hold values from -6 to 6
- base_factor: float32 [8192, 256], P(('group', 'dev')), may hold values from -0.12 to 0.12
- pivots: int32 [2, 64], replicated, may hold values from 0 to 8191, as said below
Outputs:
- new_factor: float32 [8192, 128], P(('group', 'dev'))
- residual_diag: float32 [8192], P(('group', 'dev'))
The draws below stay inside these ranges and needn't reach their ends.
Inputs may be any that keep to these rules, and one draw needn't show every extreme that they name: `pivots`: all 128 pivot indices are distinct; most of them fall on the points of a few devices.
All inputs are finite; a program needn't handle non-finite values.
Results may differ from the reference program's by a relative error of at most 0.0003.
Values sent between devices are 32-bit elements; how exact they have to be, the bound alone decides.
No kernel may reach another device: no remote copies, remote signals or barrier semaphores. Data moves between devices by JAX's collectives and lax.ppermute only.
A program may use at most 64 MiB of HBM per device.

```python
import jax
import jax.numpy as jnp
from jax import lax

DIM = 256
PIV = 64
ROUNDS = 2
BASE = 256
ROWS_DEV = 256
NPTS = 8192


def draw_points(key, part):
    values = jnp.clip(jax.random.normal(key, (NPTS, DIM), jnp.float32), -6.0, 6.0)
    return values.astype(jnp.bfloat16)


def draw_base_factor(key, part):
    values = jnp.clip(0.02 * jax.random.normal(key, (NPTS, BASE), jnp.float32), -0.12, 0.12)
    return values


def draw_pivots(key, part):
    total = ROUNDS * PIV
    owners_all = NPTS // ROWS_DEV
    local = jax.random.permutation(jax.random.fold_in(key, 11), ROWS_DEV)[:total]
    popular = jax.random.randint(jax.random.fold_in(key, 12), (4,), 0, owners_all)
    which = jax.random.randint(jax.random.fold_in(key, 13), (total,), 0, 4)
    coin = jax.random.randint(jax.random.fold_in(key, 14), (total,), 0, 4)
    anyone = jax.random.randint(jax.random.fold_in(key, 15), (total,), 0, owners_all)
    owner = jnp.where(coin < 3, popular[which], anyone)
    return (owner * ROWS_DEV + local).reshape(ROUNDS, PIV).astype(jnp.int32)


def setup_inputs(seed: int = 0) -> dict:
    keys = jax.random.split(jax.random.key(seed), 4)
    return {
        "points": draw_points(jax.random.fold_in(keys[3], 71), 0),
        "base_factor": draw_base_factor(jax.random.fold_in(keys[3], 71), 0),
        "pivots": draw_pivots(jax.random.fold_in(keys[3], 71), 0),
    }


def kernel_rows(rows, row_norms, centres, centre_norms):
    inner = jnp.dot(rows.astype(jnp.float32), centres.T.astype(jnp.float32), preferred_element_type=jnp.float32)
    dist = row_norms[:, None] + centre_norms[None, :] - 2.0 * inner
    return jnp.exp(-2.0 * dist / DIM)

def reference(points, base_factor, pivots):
    total = points.shape[0]
    norms = jnp.sum(points.astype(jnp.float32) ** 2, axis=1)
    factor = base_factor
    diag = 1.0 - jnp.sum(base_factor * base_factor, axis=1)
    collected = []
    for step in range(ROUNDS):
        chosen = pivots[step]
        centres = points[chosen]
        centre_norms = norms[chosen]
        factor_rows = factor[chosen]
        block = kernel_rows(centres, centre_norms, centres, centre_norms) - jnp.dot(factor_rows, factor_rows.T, precision=lax.Precision.HIGHEST)
        lower = jnp.linalg.cholesky(block)
        inverse = lax.linalg.triangular_solve(lower, jnp.eye(PIV, dtype=block.dtype), left_side=True, lower=True)
        width = factor.shape[1]

        def per_block(items):
            rows, row_norms, frows = items
            resid = kernel_rows(rows, row_norms, centres, centre_norms) - jnp.dot(frows, factor_rows.T, precision=lax.Precision.HIGHEST)
            return jnp.dot(resid, inverse.T, precision=lax.Precision.HIGHEST)
        blocks = total // ROWS_DEV
        cols = lax.map(per_block, (points.reshape(blocks, ROWS_DEV, DIM), norms.reshape(blocks, ROWS_DEV), factor.reshape(blocks, ROWS_DEV, width)))
        cols = cols.reshape(total, PIV)
        diag = diag - jnp.sum(cols * cols, axis=1)
        factor = jnp.concatenate([factor, cols], axis=1)
        collected.append(cols)
    return (jnp.concatenate(collected, axis=1), diag)
```

```python
import functools

import jax
import jax.numpy as jnp
from jax import lax
from jax.experimental import pallas as pl
from jax.experimental.pallas import tpu as pltpu
from jax.sharding import PartitionSpec as P

AXES = ("group", "dev")
BLOCK = 32
HIGHEST = lax.Precision.HIGHEST


def dot_nt(a, b, precision=None):
    return lax.dot_general(a, b, (((1,), (1,)), ((), ())), precision=precision, preferred_element_type=jnp.float32)


def dot_tn(a, b, precision=None):
    return lax.dot_general(a, b, (((0,), (0,)), ((), ())), precision=precision, preferred_element_type=jnp.float32)


def dot_nn(a, b, precision=None):
    return lax.dot_general(a, b, (((1,), (0,)), ((), ())), precision=precision, preferred_element_type=jnp.float32)


def pick_kernel(pivots_ref, points_ref, base_ref, mine_ref, other_ref):
    rows, dim = points_ref.shape
    half = mine_ref.shape[0]
    member = lax.axis_index("group")
    device = member * lax.axis_size("dev") + lax.axis_index("dev")
    core = member % 2
    positions = lax.broadcasted_iota(jnp.int32, (rows, half), 0) + device * rows
    points = points_ref[...]
    base = base_ref[...]
    high = base.astype(jnp.bfloat16)
    rest = base - high.astype(jnp.float32)
    middle = rest.astype(jnp.bfloat16)
    low = (rest - middle.astype(jnp.float32)).astype(jnp.bfloat16)
    for ref, which in ((mine_ref, core), (other_ref, 1 - core)):
        pivots = pivots_ref[pl.ds(which, 1), :]
        chosen = (positions == pivots).astype(jnp.bfloat16)
        ref[:, :dim] = dot_tn(chosen, points)
        ref[:, dim:] = dot_tn(chosen, high) + dot_tn(chosen, middle) + dot_tn(chosen, low)


def factor_kernel(mine_ref, other_ref, points_ref, base_ref, cols_ref, diag_ref, pivot_ref, work_ref):
    half, width = mine_ref.shape
    total = 2 * half
    rows, dim = points_ref.shape
    core = lax.axis_index("group") % 2
    pivot_ref[pl.ds(pl.multiple_of(core * half, half), half), :] = mine_ref[...]
    pivot_ref[pl.ds(pl.multiple_of((1 - core) * half, half), half), :] = other_ref[...]
    points = points_ref[...]
    base = base_ref[...]
    centres = pivot_ref[:, :dim].astype(jnp.bfloat16)
    pivot_base = pivot_ref[:, dim:]

    ones = jnp.ones((8, dim), jnp.float32)
    wide = points.astype(jnp.float32)
    norms = dot_nt(ones, wide * wide, HIGHEST)[0:1, :]
    start = 1.0 - dot_nt(ones, base * base, HIGHEST)[0:1, :]

    gram = dot_nt(centres, centres)
    eye = lax.broadcasted_iota(jnp.int32, (total, total), 0) == lax.broadcasted_iota(jnp.int32, (total, total), 1)
    own = jnp.where(eye, gram, 0.0)
    norm_lane = jnp.sum(own, axis=0, keepdims=True)
    norm_row = jnp.sum(own, axis=1, keepdims=True)
    scale = -2.0 / dim
    schur = jnp.exp(scale * (norm_row + norm_lane - 2.0 * gram)) - dot_nt(pivot_base, pivot_base, HIGHEST)
    inner = dot_nt(centres, points)
    resid = jnp.exp(scale * (norm_row + norms - 2.0 * inner)) - dot_nt(pivot_base, base, HIGHEST)
    work_ref[:, :total] = schur
    work_ref[:, total:] = resid

    b = BLOCK
    row_id = lax.broadcasted_iota(jnp.int32, (8, 128), 0)
    done = []
    for first in range(0, total, b):
        panel = [[work_ref[first + 8 * g : first + 8 * g + 8, 128 * t : 128 * t + 128] for t in range((total + rows) // 128)] for g in range(b // 8)]
        tile, lane0 = first // 128, first % 128
        rep = [
            [jnp.broadcast_to(panel[g][tile][:, lane0 + c : lane0 + c + 1], (8, 128)) if g >= c // 8 else None for g in range(b // 8)]
            for c in range(b)
        ]
        roots = [jnp.zeros((8, 128), jnp.float32) for _ in range(b // 8)]
        for j in range(b):
            gj, sj = j // 8, j % 8
            pivot = jnp.broadcast_to(rep[j][gj][sj : sj + 1, :], (8, 128))
            inverse = 1.0 / pivot
            roots[gj] = jnp.where(row_id == sj, lax.rsqrt(pivot), roots[gj])
            weight = [None] * (b // 8)
            for g in range(gj, b // 8):
                weight[g] = rep[j][g] * inverse
                if g == gj:
                    weight[g] = jnp.where(row_id > sj, weight[g], 0.0)
            for c in range(j + 1, b):
                gc, sc = c // 8, c % 8
                entry = jnp.broadcast_to(rep[j][gc][sc : sc + 1, :], (8, 128))
                for g in range(gc, b // 8):
                    rep[c][g] = rep[c][g] - weight[g] * entry
            for t in range(len(panel[0])):
                if 128 * t + 127 <= first:
                    continue
                line = jnp.broadcast_to(panel[gj][t][sj : sj + 1, :], (8, 128))
                for g in range(gj, b // 8):
                    panel[g][t] = panel[g][t] - weight[g] * line
        upper = jnp.concatenate(
            [jnp.concatenate([panel[g][t] * roots[g] for t in range(len(panel[0]))], axis=1) for g in range(b // 8)], axis=0
        )
        done.append(upper[:, total:])
        after = first + b
        if after < total:
            change = dot_tn(upper[:, :total], upper, HIGHEST)
            work_ref[after:, :] = work_ref[after:, :] - change[after:, :]
    cols = jnp.concatenate(done, axis=0)
    cols_ref[...] = cols.T
    diag_ref[...] = start - jnp.sum(cols * cols, axis=0, keepdims=True)


def exchange(mine, other, mesh):
    groups, devs = mesh.shape["group"], mesh.shape["dev"]
    half, width = mine.shape

    def swap(value, partner):
        return lax.ppermute(value, AXES, [(i, partner(i)) for i in range(groups * devs)])

    total = mine + swap(other, lambda i: i ^ devs)
    step = 1
    while step < devs:
        total = total + swap(total, lambda i: i ^ step)
        step *= 2
    step = 2
    while step < groups:
        total = total + swap(total, lambda i: i ^ (step * devs))
        step *= 2
    return total, swap(total, lambda i: i ^ devs)


def vmem(n):
    return [pl.BlockSpec(memory_space=pltpu.VMEM)] * n


def per_device(points, base_factor, pivots, mesh):
    rows, dim = points.shape
    rounds, half = pivots.shape
    base = base_factor.shape[1]
    piece = jax.ShapeDtypeStruct((half, dim + base), jnp.float32)
    mine, other = pl.pallas_call(
        pick_kernel,
        out_shape=(piece, piece),
        in_specs=vmem(3),
        out_specs=tuple(vmem(2)),
        name="pick",
    )(pivots, points, base_factor)
    mine, other = exchange(mine, other, mesh)
    total = rounds * half
    cols, diag = pl.pallas_call(
        factor_kernel,
        out_shape=(
            jax.ShapeDtypeStruct((rows, total), jnp.float32),
            jax.ShapeDtypeStruct((1, rows), jnp.float32),
        ),
        in_specs=vmem(4),
        out_specs=tuple(vmem(2)),
        scratch_shapes=[
            pltpu.VMEM((total, dim + base), jnp.float32),
            pltpu.VMEM((total, total + rows), jnp.float32),
        ],
        name="factor",
    )(mine, other, points, base_factor)
    return cols, diag.reshape(rows)


def solution(mesh):
    return jax.shard_map(
        functools.partial(per_device, mesh=mesh),
        mesh=mesh,
        in_specs=(P(AXES, None), P(AXES, None), P()),
        out_specs=(P(AXES, None), P(AXES)),
        check_vma=False,
    )
```

```python
import functools

import jax
import jax.numpy as jnp
from jax import lax
from jax.experimental import pallas as pl
from jax.experimental.pallas import tpu as pltpu
from jax.sharding import PartitionSpec as P

AXES = ("group", "dev")
WINDOW = 5


def pick_kernel(pivots_ref, points_hbm, base_hbm, *refs):
    outs, (points_ref, base_ref, sems) = refs[:-3], refs[-3:]
    copies = [pltpu.make_async_copy(points_hbm, points_ref, sems.at[0]), pltpu.make_async_copy(base_hbm, base_ref, sems.at[1])]
    for copy in copies:
        copy.start()
    rows, dim = points_ref.shape
    rounds, slots = pivots_ref.shape
    part = slots // 2
    device = lax.axis_index("group") * lax.axis_size("dev") + lax.axis_index("dev")
    first = lax.axis_index("group") % 2 == 0
    start = device * rows
    row_id = lax.broadcasted_iota(jnp.int32, (8, rows), 0)
    lane = lax.broadcasted_iota(jnp.int32, (8, rows), 1)
    chosen = []
    for r in range(rounds):
        groups = []
        for g in range(0, slots, 8):
            index = jnp.full((8, rows), pivots_ref[r, g] - start, jnp.int32)
            for k in range(1, 8):
                index = jnp.where(row_id == k, pivots_ref[r, g + k] - start, index)
            groups.append((index == lane).astype(jnp.float32))
        chosen.append(jnp.concatenate(groups, axis=0).astype(jnp.bfloat16))
    copies[0].wait()
    points = points_ref[...]
    for r in range(rounds):
        rows_of = dot(chosen[r], points, (1, 0))
        outs[2 * r][:, :dim] = jnp.where(first, rows_of[:part], rows_of[part:])
        outs[2 * r + 1][:, :dim] = jnp.where(first, rows_of[part:], rows_of[:part])
    copies[1].wait()
    high, middle, low = split(base_ref[...])
    for r in range(rounds):
        rows_of = sum(dot(chosen[r], x, (1, 0)) for x in (high, middle, low))
        outs[2 * r][:, dim:] = jnp.where(first, rows_of[:part], rows_of[part:])
        outs[2 * r + 1][:, dim:] = jnp.where(first, rows_of[part:], rows_of[:part])


def dot(a, b, dims):
    return lax.dot_general(a, b, ((dims[:1], dims[1:]), ((), ())), preferred_element_type=jnp.float32)

def split(value):
    high = value.astype(jnp.bfloat16)
    rest = value - high.astype(jnp.float32)
    middle = rest.astype(jnp.bfloat16)
    low = (rest - middle.astype(jnp.float32)).astype(jnp.bfloat16)
    return high, middle, low

def product_nt(a, b):
    n = a[0].shape[0]
    first = dot(jnp.concatenate(a, axis=0), b[0], (1, 1))
    second = dot(jnp.concatenate(a[:2], axis=0), b[1], (1, 1))
    third = dot(a[0], b[2], (1, 1))
    return first[:n] + (first[n:2*n] + second[:n]) + (first[2*n:] + second[n:] + third)

def gram_tn(upper, split_at):
    h, m, l = split(upper)
    left = jnp.concatenate([x[:, :split_at] for x in (h, m, h, l, m, h)], axis=0)
    right = jnp.concatenate([h, h, m, h, m, l], axis=0)
    return dot(left, right, (0, 0))

def spread(tile, sub):
    return jnp.broadcast_to(tile[sub:sub + 1, :], (8, 128))

def eliminate(panel, lane0):
    groups, tiles = len(panel), len(panel[0])
    b = 8 * groups
    row_id = lax.broadcasted_iota(jnp.int32, (8, 128), 0)

    def column(c):
        lane = lane0 + c
        return [jnp.broadcast_to(panel[g][0][:, lane:lane + 1], (8, 128)) if g >= c // 8 else None for g in range(groups)]

    rep = {c: column(c) for c in range(min(WINDOW + 1, b))}
    roots = [jnp.zeros((8, 128), jnp.float32) for _ in range(groups)]
    for j in range(b):
        gj, sj = j // 8, j % 8
        mine = rep.pop(j)
        pivot = spread(mine[gj], sj)
        inverse = 1.0 / pivot
        roots[gj] = jnp.where(row_id == sj, lax.rsqrt(pivot), roots[gj])
        weight = [None if g < gj else mine[g] * inverse for g in range(groups)]
        weight[gj] = jnp.where(row_id > sj, weight[gj], 0.0)
        for c in range(j + 1, min(j + WINDOW + 1, b)):
            entry = spread(mine[c // 8], c % 8)
            for g in range(c // 8, groups):
                rep[c][g] = rep[c][g] - weight[g] * entry
        for t in range(tiles):
            line = spread(panel[gj][t], sj)
            for g in range(gj, groups):
                panel[g][t] = panel[g][t] - weight[g] * line
        if j + WINDOW + 1 < b:
            rep[j + WINDOW + 1] = column(j + WINDOW + 1)
    return [[panel[g][t] * roots[g] for t in range(tiles)] for g in range(groups)]

def join(tiles):
    return jnp.concatenate([jnp.concatenate(row, axis=1) for row in tiles], axis=0)

def tiles_of(ref, row, count, tile0, tiles):
    return [[ref[row + 8 * g:row + 8 * g + 8, 128 * t:128 * t + 128] for t in range(tile0, tiles)] for g in range(count // 8)]

def factor_kernel(*refs):
    parts, (points_ref, base_ref, cols_ref, diag_ref, pivot_ref, work_ref) = refs[:-6], refs[-6:]
    part = parts[0].shape[0]
    total = part * len(parts)
    rows, dim = points_ref.shape
    core = lax.axis_index("group") % 2
    for i in range(0, len(parts), 2):
        pivot_ref[pl.ds(pl.multiple_of((i + core) * part, part), part), :] = parts[i][...]
        pivot_ref[pl.ds(pl.multiple_of((i + 1 - core) * part, part), part), :] = parts[i + 1][...]
    points = points_ref[...]
    base = base_ref[...]
    centres = pivot_ref[:, :dim].astype(jnp.bfloat16)
    pivot_base = split(pivot_ref[:, dim:])
    ones = jnp.ones((8, dim), jnp.bfloat16)
    wide = points.astype(jnp.float32)
    base_parts = split(base)
    norms = sum(dot(ones, x, (1, 1)) for x in split(wide * wide))[0:1, :]
    start = 1.0 - sum(dot(ones, x, (1, 1)) for x in split(base * base))[0:1, :]
    gram = dot(centres, centres, (1, 1))
    eye = lax.broadcasted_iota(jnp.int32, (total, total), 0) == lax.broadcasted_iota(jnp.int32, (total, total), 1)
    own = jnp.where(eye, gram, 0.0)
    norm_lane = jnp.sum(own, axis=0, keepdims=True)
    norm_row = jnp.sum(own, axis=1, keepdims=True)
    scale = -2.0 / dim
    work_ref[:, :total] = jnp.exp(scale * (norm_row + norm_lane - 2.0 * gram)) - product_nt(pivot_base, pivot_base)
    inner = dot(centres, points, (1, 1))
    work_ref[:, total:] = jnp.exp(scale * (norm_row + norms - 2.0 * inner)) - product_nt(pivot_base, base_parts)
    half = total // 2
    count = (total + rows) // 128
    top = join(eliminate(tiles_of(work_ref, 0, half, 0, count), 0))
    work_ref[half:, :] = work_ref[half:, :] - gram_tn(top, total)[half:, :]
    bottom = join(eliminate(tiles_of(work_ref, half, half, 0, count), half))
    cols = jnp.concatenate([top[:, total:], bottom[:, total:]], axis=0)
    cols_ref[...] = cols.T
    diag_ref[...] = start - jnp.sum(cols * cols, axis=0, keepdims=True)


def exchange(chains, mesh):
    groups, devs = mesh.shape["group"], mesh.shape["dev"]

    def swap(value, partner):
        return lax.ppermute(value, AXES, [(i, partner(i)) for i in range(groups * devs)])

    def add(a, b):
        return a + b

    near = [1 << k for k in range(devs.bit_length() - 1)]
    far = [devs << k for k in range(1, groups.bit_length() - 1)]
    assert 1 << len(near) == devs and 2 << len(far) == groups
    steps = near[:1] + far + near[1:]
    turn = len(steps) // 2
    orders = (steps, steps[turn:] + steps[:turn])
    got = [swap(chains[2 * r + 1], lambda i: i ^ devs) for r in range(2)]
    sums = [add(chains[2 * r], got[r]) for r in range(2)]
    for k in range(len(steps)):
        got = [swap(sums[r], lambda i: i ^ orders[r][k]) for r in range(2)]
        sums = [add(sums[r], got[r]) for r in range(2)]
    k = len(steps) + 1
    got = [swap(sums[r], lambda i: i ^ devs) for r in range(2)]
    return sums[0], got[0], sums[1], got[1]


def vmem(n):
    return [pl.BlockSpec(memory_space=pltpu.VMEM)] * n


def per_device(points, base_factor, pivots, mesh):
    rows, dim = points.shape
    rounds, slots = pivots.shape
    base = base_factor.shape[1]
    piece = jax.ShapeDtypeStruct((slots // 2, dim + base), jnp.float32)
    n = 2 * rounds
    chains = pl.pallas_call(
        pick_kernel,
        out_shape=(piece,) * n,
        in_specs=[pl.BlockSpec(memory_space=pltpu.SMEM)] + [pl.BlockSpec(memory_space=pl.ANY)] * 2,
        out_specs=tuple(vmem(n)),
        scratch_shapes=[
            pltpu.VMEM(points.shape, points.dtype),
            pltpu.VMEM(base_factor.shape, base_factor.dtype),
            pltpu.SemaphoreType.DMA((2,)),
        ],
        compiler_params=pltpu.CompilerParams(vmem_limit_bytes=54900 * 1024),
        name="pick",
    )(pivots, points, base_factor)
    parts = exchange(chains, mesh)
    total = rounds * slots
    cols, diag = pl.pallas_call(
        factor_kernel,
        out_shape=(
            jax.ShapeDtypeStruct((rows, total), jnp.float32),
            jax.ShapeDtypeStruct((1, rows), jnp.float32),
        ),
        in_specs=vmem(n + 2),
        out_specs=tuple(vmem(2)),
        scratch_shapes=[
            pltpu.VMEM((total, dim + base), jnp.float32),
            pltpu.VMEM((total, total + rows), jnp.float32),
        ],
        compiler_params=pltpu.CompilerParams(vmem_limit_bytes=16 * 2**20),
        name="factor",
    )(*parts, points, base_factor)
    return cols, diag.reshape(rows)


def solution(mesh):
    return jax.shard_map(
        functools.partial(per_device, mesh=mesh),
        mesh=mesh,
        in_specs=(P(AXES, None), P(AXES, None), P()),
        out_specs=(P(AXES, None), P(AXES)),
        check_vma=False,
    )
```

```python
import functools

import jax
import jax.numpy as jnp
from jax import lax
from jax.experimental import pallas as pl
from jax.experimental.pallas import tpu as pltpu
from jax.sharding import PartitionSpec as P

AXES = ("group", "dev")
WINDOW = 5


def pick_kernel(pivots_ref, points_hbm, base_hbm, *refs):
    outs, local, (base_ref, sems) = refs[:-8], refs[-8:-2], refs[-2:]
    points_ref, high_ref, middle_ref, low_ref, norms_ref, start_ref = local
    copies = [pltpu.make_async_copy(points_hbm, points_ref, sems.at[0]), pltpu.make_async_copy(base_hbm, base_ref, sems.at[1])]
    for copy in copies:
        copy.start()
    rows, dim = points_ref.shape
    rounds, slots = pivots_ref.shape
    part = slots // 2
    device = lax.axis_index("group") * lax.axis_size("dev") + lax.axis_index("dev")
    first = lax.axis_index("group") % 2 == 0
    positions = lax.broadcasted_iota(jnp.int32, (rows, slots), 0) + device * rows
    chosen = [(positions == pivots_ref[r : r + 1, :]).astype(jnp.bfloat16) for r in range(rounds)]
    ones = jnp.ones((8, dim), jnp.bfloat16)

    def put(lanes, pieces):
        for r in range(rounds):
            rows_of = sum(dot(chosen[r], piece, (0, 0)) for piece in pieces)
            outs[2 * r][:, lanes] = jnp.where(first, rows_of[:part], rows_of[part:])
            outs[2 * r + 1][:, lanes] = jnp.where(first, rows_of[part:], rows_of[:part])

    copies[0].wait()
    points = points_ref[...]
    put(slice(0, dim), (points,))
    wide = points.astype(jnp.float32)
    norms_ref[...] = sum(dot(ones, x, (1, 1)) for x in split(wide * wide)[:2])[0:1, :]
    copies[1].wait()
    base = base_ref[...]
    parts = split(base)
    put(slice(dim, None), parts)
    high_ref[...], middle_ref[...], low_ref[...] = parts
    start_ref[...] = 1.0 - sum(dot(ones, x, (1, 1)) for x in split(base * base))[0:1, :]


def dot(a, b, dims):
    return lax.dot_general(a, b, ((dims[:1], dims[1:]), ((), ())), preferred_element_type=jnp.float32)

def split(value):
    high = value.astype(jnp.bfloat16)
    rest = value - high.astype(jnp.float32)
    middle = rest.astype(jnp.bfloat16)
    low = (rest - middle.astype(jnp.float32)).astype(jnp.bfloat16)
    return high, middle, low

def product_nt(a, b):
    n = a[0].shape[0]
    first = dot(jnp.concatenate(a, axis=0), b[0], (1, 1))
    second = dot(jnp.concatenate(a[:2], axis=0), b[1], (1, 1))
    third = dot(a[0], b[2], (1, 1))
    return first[:n] + (first[n:2*n] + second[:n]) + (first[2*n:] + second[n:] + third)

def gram_tn(upper, split_at):
    h, m, l = split(upper)
    left = jnp.concatenate([x[:, :split_at] for x in (h, m, h, l, m, h)], axis=0)
    right = jnp.concatenate([h, h, m, h, m, l], axis=0)
    return dot(left, right, (0, 0))

def spread(tile, sub):
    return jnp.broadcast_to(tile[sub:sub + 1, :], (8, 128))

def eliminate(panel, lane0):
    groups, tiles = len(panel), len(panel[0])
    b = 8 * groups
    row_id = lax.broadcasted_iota(jnp.int32, (8, 128), 0)

    def column(c):
        lane = lane0 + c
        return [jnp.broadcast_to(panel[g][0][:, lane:lane + 1], (8, 128)) if g >= c // 8 else None for g in range(groups)]

    rep = {c: column(c) for c in range(min(WINDOW + 1, b))}
    roots = [jnp.zeros((8, 128), jnp.float32) for _ in range(groups)]
    for j in range(b):
        gj, sj = j // 8, j % 8
        mine = rep.pop(j)
        pivot = spread(mine[gj], sj)
        inverse = 1.0 / pivot
        roots[gj] = jnp.where(row_id == sj, lax.rsqrt(pivot), roots[gj])
        weight = [None if g < gj else mine[g] * inverse for g in range(groups)]
        weight[gj] = jnp.where(row_id > sj, weight[gj], 0.0)
        for c in range(j + 1, min(j + WINDOW + 1, b)):
            entry = spread(mine[c // 8], c % 8)
            for g in range(c // 8, groups):
                rep[c][g] = rep[c][g] - weight[g] * entry
        for t in range(tiles):
            line = spread(panel[gj][t], sj)
            for g in range(gj, groups):
                panel[g][t] = panel[g][t] - weight[g] * line
        if j + WINDOW + 1 < b:
            rep[j + WINDOW + 1] = column(j + WINDOW + 1)
    return [[panel[g][t] * roots[g] for t in range(tiles)] for g in range(groups)]

def join(tiles):
    return jnp.concatenate([jnp.concatenate(row, axis=1) for row in tiles], axis=0)

def tiles_of(ref, row, count, tile0, tiles):
    return [[ref[row + 8 * g:row + 8 * g + 8, 128 * t:128 * t + 128] for t in range(tile0, tiles)] for g in range(count // 8)]

def factor_kernel(*refs):
    parts, local, (cols_ref, diag_ref, pivot_ref, work_ref) = refs[:-10], refs[-10:-4], refs[-4:]
    points_ref, high_ref, middle_ref, low_ref, norms_ref, start_ref = local
    part = parts[0].shape[0]
    total = part * len(parts)
    rows, dim = points_ref.shape
    core = lax.axis_index("group") % 2
    for i in range(0, len(parts), 2):
        pivot_ref[pl.ds(pl.multiple_of((i + core) * part, part), part), :] = parts[i][...]
        pivot_ref[pl.ds(pl.multiple_of((i + 1 - core) * part, part), part), :] = parts[i + 1][...]
    points = points_ref[...]
    base_parts = high_ref[...], middle_ref[...], low_ref[...]
    norms = norms_ref[...]
    centres = pivot_ref[:, :dim].astype(jnp.bfloat16)
    pivot_base = split(pivot_ref[:, dim:])
    gram = dot(centres, centres, (1, 1))
    eye = lax.broadcasted_iota(jnp.int32, (total, total), 0) == lax.broadcasted_iota(jnp.int32, (total, total), 1)
    own = jnp.where(eye, gram, 0.0)
    norm_lane = jnp.sum(own, axis=0, keepdims=True)
    norm_row = jnp.sum(own, axis=1, keepdims=True)
    scale = -2.0 / dim
    work_ref[:, :total] = jnp.exp(scale * (norm_row + norm_lane - 2.0 * gram)) - product_nt(pivot_base, pivot_base)
    inner = dot(centres, points, (1, 1))
    work_ref[:, total:] = jnp.exp(scale * (norm_row + norms - 2.0 * inner)) - product_nt(pivot_base, base_parts)
    half = total // 2
    count = (total + rows) // 128
    top = join(eliminate(tiles_of(work_ref, 0, half, 0, count), 0))
    work_ref[half:, :] = work_ref[half:, :] - gram_tn(top, total)[half:, :]
    bottom = join(eliminate(tiles_of(work_ref, half, half, 0, count), half))
    cols = jnp.concatenate([top[:, total:], bottom[:, total:]], axis=0)
    cols_ref[...] = cols.T
    diag_ref[...] = start_ref[...] - jnp.sum(cols * cols, axis=0, keepdims=True)


def exchange(chains, mesh):
    groups, devs = mesh.shape["group"], mesh.shape["dev"]

    def swap(value, partner):
        return lax.ppermute(value, AXES, [(i, partner(i)) for i in range(groups * devs)])

    def add(a, b):
        return a + b

    near = [1 << k for k in range(devs.bit_length() - 1)]
    far = [devs << k for k in range(1, groups.bit_length() - 1)]
    assert 1 << len(near) == devs and 2 << len(far) == groups
    steps = near[:1] + far + near[1:]
    turn = len(steps) // 2
    orders = (steps, steps[turn:] + steps[:turn])
    got = [swap(chains[2 * r + 1], lambda i: i ^ devs) for r in range(2)]
    sums = [add(chains[2 * r], got[r]) for r in range(2)]
    for k in range(len(steps)):
        got = [swap(sums[r], lambda i: i ^ orders[r][k]) for r in range(2)]
        sums = [add(sums[r], got[r]) for r in range(2)]
    k = len(steps) + 1
    got = [swap(sums[r], lambda i: i ^ devs) for r in range(2)]
    return sums[0], got[0], sums[1], got[1]


def vmem(n):
    return [pl.BlockSpec(memory_space=pltpu.VMEM)] * n


def per_device(points, base_factor, pivots, mesh):
    rows, dim = points.shape
    rounds, slots = pivots.shape
    base = base_factor.shape[1]
    piece = jax.ShapeDtypeStruct((slots // 2, dim + base), jnp.float32)
    n = 2 * rounds
    chains = pl.pallas_call(
        pick_kernel,
        out_shape=(piece,) * n
        + (jax.ShapeDtypeStruct(points.shape, points.dtype),)
        + (jax.ShapeDtypeStruct(base_factor.shape, jnp.bfloat16),) * 3
        + (jax.ShapeDtypeStruct((1, rows), jnp.float32),) * 2,
        in_specs=vmem(1) + [pl.BlockSpec(memory_space=pl.ANY)] * 2,
        out_specs=tuple(vmem(n + 6)),
        scratch_shapes=[pltpu.VMEM(base_factor.shape, base_factor.dtype), pltpu.SemaphoreType.DMA((2,))],
        compiler_params=pltpu.CompilerParams(vmem_limit_bytes=54380 * 1024),
        name="pick",
    )(pivots, points, base_factor)
    chains, local = chains[:n], chains[n:]
    parts = exchange(chains, mesh)
    total = rounds * slots
    cols, diag = pl.pallas_call(
        factor_kernel,
        out_shape=(
            jax.ShapeDtypeStruct((rows, total), jnp.float32),
            jax.ShapeDtypeStruct((1, rows), jnp.float32),
        ),
        in_specs=vmem(n + 6),
        out_specs=tuple(vmem(2)),
        scratch_shapes=[
            pltpu.VMEM((total, dim + base), jnp.float32),
            pltpu.VMEM((total, total + rows), jnp.float32),
        ],
        compiler_params=pltpu.CompilerParams(vmem_limit_bytes=16 * 2**20),
        name="factor",
    )(*parts, *local)
    return cols, diag.reshape(rows)


def solution(mesh):
    return jax.shard_map(
        functools.partial(per_device, mesh=mesh),
        mesh=mesh,
        in_specs=(P(AXES, None), P(AXES, None), P()),
        out_specs=(P(AXES, None), P(AXES)),
        check_vma=False,
    )
```

```python
import functools

import jax
import jax.numpy as jnp
from jax import lax
from jax.experimental import pallas as pl
from jax.experimental.pallas import tpu as pltpu
from jax.sharding import PartitionSpec as P

AXES = ("group", "dev")


def pick_kernel(pivots_ref, points_hbm, base_hbm, *refs):
    outs, local, (base_ref, sems) = refs[:-8], refs[-8:-2], refs[-2:]
    points_ref, high_ref, middle_ref, low_ref, norms_ref, start_ref = local
    copies = [pltpu.make_async_copy(points_hbm, points_ref, sems.at[0]), pltpu.make_async_copy(base_hbm, base_ref, sems.at[1])]
    for copy in copies:
        copy.start()
    rows, dim = points_ref.shape
    rounds, slots = pivots_ref.shape
    part = slots // 2
    device = lax.axis_index("group") * lax.axis_size("dev") + lax.axis_index("dev")
    first = lax.axis_index("group") % 2 == 0
    positions = lax.broadcasted_iota(jnp.int32, (rows, slots), 0) + device * rows
    chosen = [(positions == pivots_ref[r : r + 1, :]).astype(jnp.bfloat16) for r in range(rounds)]
    ones = jnp.ones((8, dim), jnp.bfloat16)

    def put(lanes, pieces):
        for r in range(rounds):
            rows_of = sum(dot(chosen[r], piece, (0, 0)) for piece in pieces)
            outs[2 * r][:, lanes] = jnp.where(first, rows_of[:part], rows_of[part:])
            outs[2 * r + 1][:, lanes] = jnp.where(first, rows_of[part:], rows_of[:part])

    copies[0].wait()
    points = points_ref[...]
    put(slice(0, dim), (points,))
    wide = points.astype(jnp.float32)
    norms_ref[...] = sum(dot(ones, x, (1, 1)) for x in split(wide * wide)[:2])[0:1, :]
    copies[1].wait()
    base = base_ref[...]
    parts = split(base)
    put(slice(dim, None), parts)
    high_ref[...], middle_ref[...], low_ref[...] = parts
    start_ref[...] = 1.0 - sum(dot(ones, x, (1, 1)) for x in split(base * base))[0:1, :]


def dot(a, b, dims):
    return lax.dot_general(a, b, ((dims[:1], dims[1:]), ((), ())), preferred_element_type=jnp.float32)


def split(value):
    high = value.astype(jnp.bfloat16)
    rest = value - high.astype(jnp.float32)
    middle = rest.astype(jnp.bfloat16)
    low = (rest - middle.astype(jnp.float32)).astype(jnp.bfloat16)
    return high, middle, low


def product_nt(a, b):
    n = a[0].shape[0]
    first = dot(jnp.concatenate(a, axis=0), b[0], (1, 1))
    second = dot(jnp.concatenate(a[:2], axis=0), b[1], (1, 1))
    third = dot(a[0], b[2], (1, 1))
    return first[:n] + (first[n:2*n] + second[:n]) + (first[2*n:] + second[n:] + third)


def terms(value, axis, left):
    h, m, l = split(value)
    return jnp.concatenate((h, m, h, l, m, h) if left else (h, h, m, h, m, l), axis=axis)


def ahead(column):
    return 4 + column // 12


def spread(tile, sub):
    return jnp.broadcast_to(tile[sub:sub + 1, :], (8, 128))


def eliminate(panel, lane0):
    groups, tiles = len(panel), len(panel[0])
    b = 8 * groups
    row_id = lax.broadcasted_iota(jnp.int32, (8, 128), 0)

    def column(c):
        lane = lane0 + c
        return [jnp.broadcast_to(panel[g][0][:, lane : lane + 1], (8, 128)) if g >= c // 8 else None for g in range(groups)]

    rep = {}
    fresh = 0
    roots = [jnp.zeros((8, 128), jnp.float32) for _ in range(groups)]
    for j in range(b):
        while fresh < b and fresh - ahead(fresh) <= j:
            rep[fresh] = column(fresh)
            fresh += 1
        gj, sj = j // 8, j % 8
        mine = rep.pop(j)
        pivot = spread(mine[gj], sj)
        inverse = 1.0 / pivot
        roots[gj] = jnp.where(row_id == sj, lax.rsqrt(pivot), roots[gj])
        weight = [None if g < gj else mine[g] * inverse for g in range(groups)]
        weight[gj] = jnp.where(row_id > sj, weight[gj], 0.0)
        for c in sorted(rep):
            entry = spread(mine[c // 8], c % 8)
            for g in range(c // 8, groups):
                rep[c][g] = rep[c][g] - weight[g] * entry
        for t in range(tiles):
            line = spread(panel[gj][t], sj)
            for g in range(gj, groups):
                panel[g][t] = panel[g][t] - weight[g] * line
    return [[panel[g][t] * roots[g] for t in range(tiles)] for g in range(groups)]


def join(tiles):
    return jnp.concatenate([jnp.concatenate(row, axis=1) for row in tiles], axis=0)


def tiles_of(ref, row, count, tile0, tiles):
    return [[ref[row + 8 * g:row + 8 * g + 8, 128 * t:128 * t + 128] for t in range(tile0, tiles)] for g in range(count // 8)]


def kernel_rows(inner, row_norms, lane_norms, dim):
    return jnp.exp((-2.0 / dim) * (row_norms + lane_norms - 2.0 * inner))


def gather_rows(target, mine, other):
    part = mine.shape[0]
    core = lax.axis_index("group") % 2
    target[pl.ds(pl.multiple_of(core * part, part), part), :] = mine[...]
    target[pl.ds(pl.multiple_of((1 - core) * part, part), part), :] = other[...]


def first_kernel(mine, other, points_ref, high_ref, middle_ref, low_ref, norms_ref, centres_ref, pieces_ref, norm_ref, inverse_ref, cols_ref, rows_ref, work_ref):
    gather_rows(rows_ref, mine, other)
    dim = points_ref.shape[1]
    size = rows_ref.shape[0]
    centres = rows_ref[:, :dim].astype(jnp.bfloat16)
    pieces = split(rows_ref[:, dim:])
    centres_ref[...] = centres
    pieces_ref[...] = jnp.concatenate(pieces, axis=0)
    gram = dot(centres, centres, (1, 1))
    eye = lax.broadcasted_iota(jnp.int32, (size, size), 0) == lax.broadcasted_iota(jnp.int32, (size, size), 1)
    own = jnp.where(eye, gram, 0.0)
    norm_lane = jnp.sum(own, axis=0, keepdims=True)
    norm_row = jnp.broadcast_to(jnp.sum(own, axis=1, keepdims=True), (size, 128))
    norm_ref[...] = norm_row
    work_ref[:, :size] = kernel_rows(gram, norm_row[:, :1], norm_lane, dim) - product_nt(pieces, pieces)
    work_ref[:, size : 2 * size] = eye.astype(jnp.float32)
    inner = dot(centres, points_ref[...], (1, 1))
    base = high_ref[...], middle_ref[...], low_ref[...]
    work_ref[:, 128:] = kernel_rows(inner, norm_row[:, :1], norms_ref[...], dim) - product_nt(pieces, base)
    upper = join(eliminate(tiles_of(work_ref, 0, size, 0, work_ref.shape[1] // 128), 0))
    inverse_ref[...] = terms(upper[:, size : 2 * size], 1, True)
    cols_ref[...] = upper[:, 128:]


def second_kernel(mine, other, points_ref, high_ref, middle_ref, low_ref, norms_ref, start_ref, centres_ref, pieces_ref, norm_ref, inverse_ref, before_ref, cols_ref, diag_ref, rows_ref, work_ref):
    gather_rows(rows_ref, mine, other)
    dim = points_ref.shape[1]
    size = rows_ref.shape[0]
    centres = rows_ref[:, :dim].astype(jnp.bfloat16)
    pieces = split(rows_ref[:, dim:])
    before = before_ref[...]
    old = tuple(pieces_ref[k * size : (k + 1) * size, :] for k in range(3))
    cross = dot(centres_ref[...], centres, (1, 1))
    gram = dot(centres, centres, (1, 1))
    eye = lax.broadcasted_iota(jnp.int32, (size, size), 0) == lax.broadcasted_iota(jnp.int32, (size, size), 1)
    own = jnp.where(eye, gram, 0.0)
    norm_lane = jnp.sum(own, axis=0, keepdims=True)
    norm_row = jnp.sum(own, axis=1, keepdims=True)
    cross = kernel_rows(cross, norm_ref[...][:, :1], norm_lane, dim) - product_nt(old, pieces)
    share = dot(inverse_ref[...], terms(cross, 0, False), (1, 0))
    block = kernel_rows(gram, norm_row, norm_lane, dim) - product_nt(pieces, pieces)
    inner = dot(centres, points_ref[...], (1, 1))
    base = high_ref[...], middle_ref[...], low_ref[...]
    resid = kernel_rows(inner, norm_row, norms_ref[...], dim) - product_nt(pieces, base)
    left = terms(share, 0, True)
    work_ref[:, :size] = block - dot(left, terms(share, 0, False), (0, 0))
    work_ref[:, size : 2 * size] = eye.astype(jnp.float32)
    work_ref[:, 128:] = resid - dot(left, terms(before, 0, False), (0, 0))
    upper = join(eliminate(tiles_of(work_ref, 0, size, 0, work_ref.shape[1] // 128), 0))
    cols = jnp.concatenate([before, upper[:, 128:]], axis=0)
    cols_ref[...] = cols.T
    diag_ref[...] = start_ref[...] - jnp.sum(cols * cols, axis=0, keepdims=True)


def exchange(chains, mesh):
    groups, devs = mesh.shape["group"], mesh.shape["dev"]

    def swap(value, partner):
        return lax.ppermute(value, AXES, [(i, partner(i)) for i in range(groups * devs)])

    def add(a, b):
        return a + b

    near = [1 << k for k in range(devs.bit_length() - 1)]
    far = [devs << k for k in range(1, groups.bit_length() - 1)]
    assert 1 << len(near) == devs and 2 << len(far) == groups
    steps = near[:1] + far + near[1:]
    turn = len(steps) // 2
    orders = (steps, steps[turn:] + steps[:turn])
    got = [swap(chains[2 * r + 1], lambda i: i ^ devs) for r in range(2)]
    sums = [add(chains[2 * r], got[r]) for r in range(2)]
    for k in range(len(steps)):
        got = [swap(sums[r], lambda i: i ^ orders[r][k]) for r in range(2)]
        sums = [add(sums[r], got[r]) for r in range(2)]
    k = len(steps) + 1
    got = [swap(sums[r], lambda i: i ^ devs) for r in range(2)]
    return sums[0], got[0], sums[1], got[1]


def vmem(n):
    return [pl.BlockSpec(memory_space=pltpu.VMEM)] * n


def per_device(points, base_factor, pivots, mesh):
    rows, dim = points.shape
    rounds, slots = pivots.shape
    base = base_factor.shape[1]
    piece = jax.ShapeDtypeStruct((slots // 2, dim + base), jnp.float32)
    n = 2 * rounds
    chains = pl.pallas_call(
        pick_kernel,
        out_shape=(piece,) * n
        + (jax.ShapeDtypeStruct(points.shape, points.dtype),)
        + (jax.ShapeDtypeStruct(base_factor.shape, jnp.bfloat16),) * 3
        + (jax.ShapeDtypeStruct((1, rows), jnp.float32),) * 2,
        in_specs=vmem(1) + [pl.BlockSpec(memory_space=pl.ANY)] * 2,
        out_specs=tuple(vmem(n + 6)),
        scratch_shapes=[pltpu.VMEM(base_factor.shape, base_factor.dtype), pltpu.SemaphoreType.DMA((2,))],
        compiler_params=pltpu.CompilerParams(vmem_limit_bytes=54380 * 1024),
        name="pick",
    )(pivots, points, base_factor)
    chains, local = chains[:n], chains[n:]
    parts = exchange(chains, mesh)
    width = dim + base
    half = jnp.bfloat16
    scratch = [pltpu.VMEM((slots, width), jnp.float32), pltpu.VMEM((slots, 128 + rows), jnp.float32)]
    front = pl.pallas_call(
        first_kernel,
        out_shape=(
            jax.ShapeDtypeStruct((slots, dim), half),
            jax.ShapeDtypeStruct((3 * slots, base), half),
            jax.ShapeDtypeStruct((slots, 128), jnp.float32),
            jax.ShapeDtypeStruct((slots, 6 * slots), half),
            jax.ShapeDtypeStruct((slots, rows), jnp.float32),
        ),
        in_specs=vmem(7),
        out_specs=tuple(vmem(5)),
        scratch_shapes=scratch,
        compiler_params=pltpu.CompilerParams(vmem_limit_bytes=16 * 2**20),
        cost_estimate=pl.CostEstimate(flops=10**7, bytes_accessed=2**19, transcendentals=0),
        name="first",
    )(*parts[:2], *local[:5])
    cols, diag = pl.pallas_call(
        second_kernel,
        out_shape=(
            jax.ShapeDtypeStruct((rows, 2 * slots), jnp.float32),
            jax.ShapeDtypeStruct((1, rows), jnp.float32),
        ),
        in_specs=vmem(13),
        out_specs=tuple(vmem(2)),
        scratch_shapes=scratch,
        compiler_params=pltpu.CompilerParams(vmem_limit_bytes=16 * 2**20),
        name="second",
    )(*parts[2:], *local, *front)
    return cols, diag.reshape(rows)


def solution(mesh):
    return jax.shard_map(
        functools.partial(per_device, mesh=mesh),
        mesh=mesh,
        in_specs=(P(AXES, None), P(AXES, None), P()),
        out_specs=(P(AXES, None), P(AXES)),
        check_vma=False,
    )
```

```python
import functools

import jax
import jax.numpy as jnp
from jax import lax
from jax.experimental import pallas as pl
from jax.experimental.pallas import tpu as pltpu
from jax.sharding import PartitionSpec as P


AXES = ("group", "dev")


def pick_kernel(pivots_ref, points_hbm, base_hbm, *refs):
    outs, local, (base_ref, sems) = refs[:-8], refs[-8:-2], refs[-2:]
    points_ref, high_ref, middle_ref, low_ref, norms_ref, start_ref = local
    copies = [pltpu.make_async_copy(points_hbm, points_ref, sems.at[0]), pltpu.make_async_copy(base_hbm, base_ref, sems.at[1])]
    for copy in copies:
        copy.start()
    rows, dim = points_ref.shape
    rounds, slots = pivots_ref.shape
    part = slots // 2
    device = lax.axis_index("group") * lax.axis_size("dev") + lax.axis_index("dev")
    first = lax.axis_index("group") % 2 == 0
    positions = lax.broadcasted_iota(jnp.int32, (rows, slots), 0) + device * rows
    chosen = [(positions == pivots_ref[r : r + 1, :]).astype(jnp.bfloat16) for r in range(rounds)]
    ones = jnp.ones((8, dim), jnp.bfloat16)

    def put(lanes, pieces):
        for r in range(rounds):
            rows_of = sum(dot(chosen[r], piece, (0, 0)) for piece in pieces)
            outs[2 * r][:, lanes] = jnp.where(first, rows_of[:part], rows_of[part:])
            outs[2 * r + 1][:, lanes] = jnp.where(first, rows_of[part:], rows_of[:part])

    copies[0].wait()
    points = points_ref[...]
    put(slice(0, dim), (points,))
    wide = points.astype(jnp.float32)
    norms_ref[...] = sum(dot(ones, x, (1, 1)) for x in split(wide * wide)[:2])[0:1, :]
    copies[1].wait()
    base = base_ref[...]
    parts = split(base)
    put(slice(dim, None), parts)
    high_ref[...], middle_ref[...], low_ref[...] = parts
    start_ref[...] = 1.0 - sum(dot(ones, x, (1, 1)) for x in split(base * base))[0:1, :]


def dot(a, b, dims):
    return lax.dot_general(a, b, ((dims[:1], dims[1:]), ((), ())), preferred_element_type=jnp.float32)


def split(value):
    high = value.astype(jnp.bfloat16)
    rest = value - high.astype(jnp.float32)
    middle = rest.astype(jnp.bfloat16)
    low = (rest - middle.astype(jnp.float32)).astype(jnp.bfloat16)
    return high, middle, low


def product_nt(a, b):
    n = a[0].shape[0]
    first = dot(jnp.concatenate(a, axis=0), b[0], (1, 1))
    second = dot(jnp.concatenate(a[:2], axis=0), b[1], (1, 1))
    third = dot(a[0], b[2], (1, 1))
    return first[:n] + (first[n:2*n] + second[:n]) + (first[2*n:] + second[n:] + third)


def terms(value, axis, left):
    h, m, l = split(value)
    return jnp.concatenate((h, m, h, l, m, h) if left else (h, h, m, h, m, l), axis=axis)


def ahead(column):
    return 4 + column // 12


def spread(tile, sub):
    return jnp.broadcast_to(tile[sub:sub + 1, :], (8, 128))


def eliminate(panel, lane0):
    groups, tiles = len(panel), len(panel[0])
    b = 8 * groups
    row_id = lax.broadcasted_iota(jnp.int32, (8, 128), 0)

    def column(c):
        lane = lane0 + c
        return [jnp.broadcast_to(panel[g][0][:, lane : lane + 1], (8, 128)) if g >= c // 8 else None for g in range(groups)]

    rep = {}
    fresh = 0
    roots = [jnp.zeros((8, 128), jnp.float32) for _ in range(groups)]
    for j in range(b):
        while fresh < b and fresh - ahead(fresh) <= j:
            rep[fresh] = column(fresh)
            fresh += 1
        gj, sj = j // 8, j % 8
        mine = rep.pop(j)
        pivot = spread(mine[gj], sj)
        inverse = 1.0 / pivot
        roots[gj] = jnp.where(row_id == sj, lax.rsqrt(pivot), roots[gj])
        weight = [None if g < gj else mine[g] * inverse for g in range(groups)]
        weight[gj] = jnp.where(row_id > sj, weight[gj], 0.0)
        for c in sorted(rep):
            entry = spread(mine[c // 8], c % 8)
            for g in range(c // 8, groups):
                rep[c][g] = rep[c][g] - weight[g] * entry
        for t in range(tiles):
            line = spread(panel[gj][t], sj)
            for g in range(gj, groups):
                panel[g][t] = panel[g][t] - weight[g] * line
    return [[panel[g][t] * roots[g] for t in range(tiles)] for g in range(groups)]


def join(tiles):
    return jnp.concatenate([jnp.concatenate(row, axis=1) for row in tiles], axis=0)


def tiles_of(ref, row, count, tile0, tiles):
    return [[ref[row + 8 * g:row + 8 * g + 8, 128 * t:128 * t + 128] for t in range(tile0, tiles)] for g in range(count // 8)]


def kernel_rows(inner, row_norms, lane_norms, dim):
    return jnp.exp((-2.0 / dim) * (row_norms + lane_norms - 2.0 * inner))


def gather_rows(target, mine, other):
    part = mine.shape[0]
    core = lax.axis_index("group") % 2
    target[pl.ds(pl.multiple_of(core * part, part), part), :] = mine[...]
    target[pl.ds(pl.multiple_of((1 - core) * part, part), part), :] = other[...]


def zero_kernel(mine, other, points_ref, high_ref, middle_ref, low_ref, norms_ref, centres_ref, pieces_ref, norm_ref, work_ref, rows_ref):
    gather_rows(rows_ref, mine, other)
    dim = points_ref.shape[1]
    size = rows_ref.shape[0]
    centres = rows_ref[:, :dim].astype(jnp.bfloat16)
    pieces = split(rows_ref[:, dim:])
    centres_ref[...] = centres
    pieces_ref[...] = jnp.concatenate(pieces, axis=0)
    gram = dot(centres, centres, (1, 1))
    eye = lax.broadcasted_iota(jnp.int32, (size, size), 0) == lax.broadcasted_iota(jnp.int32, (size, size), 1)
    own = jnp.where(eye, gram, 0.0)
    norm_lane = jnp.sum(own, axis=0, keepdims=True)
    norm_row = jnp.broadcast_to(jnp.sum(own, axis=1, keepdims=True), (size, 128))
    norm_ref[...] = norm_row
    work_ref[:, :size] = kernel_rows(gram, norm_row[:, :1], norm_lane, dim) - product_nt(pieces, pieces)
    work_ref[:, size : 2 * size] = eye.astype(jnp.float32)
    inner = dot(centres, points_ref[...], (1, 1))
    base = high_ref[...], middle_ref[...], low_ref[...]
    work_ref[:, 128:] = kernel_rows(inner, norm_row[:, :1], norms_ref[...], dim) - product_nt(pieces, base)


def first_kernel(work_ref, inverse_ref, cols_ref):
    size = work_ref.shape[0]
    upper = join(eliminate(tiles_of(work_ref, 0, size, 0, work_ref.shape[1] // 128), 0))
    inverse_ref[...] = terms(upper[:, size : 2 * size], 1, True)
    cols_ref[...] = upper[:, 128:]


def second_kernel(mine, other, points_ref, high_ref, middle_ref, low_ref, norms_ref, start_ref, centres_ref, pieces_ref, norm_ref, inverse_ref, before_ref, cols_ref, diag_ref, rows_ref, work_ref):
    gather_rows(rows_ref, mine, other)
    dim = points_ref.shape[1]
    size = rows_ref.shape[0]
    centres = rows_ref[:, :dim].astype(jnp.bfloat16)
    pieces = split(rows_ref[:, dim:])
    before = before_ref[...]
    old = tuple(pieces_ref[k * size : (k + 1) * size, :] for k in range(3))
    cross = dot(centres_ref[...], centres, (1, 1))
    gram = dot(centres, centres, (1, 1))
    eye = lax.broadcasted_iota(jnp.int32, (size, size), 0) == lax.broadcasted_iota(jnp.int32, (size, size), 1)
    own = jnp.where(eye, gram, 0.0)
    norm_lane = jnp.sum(own, axis=0, keepdims=True)
    norm_row = jnp.sum(own, axis=1, keepdims=True)
    cross = kernel_rows(cross, norm_ref[...][:, :1], norm_lane, dim) - product_nt(old, pieces)
    share = dot(inverse_ref[...], terms(cross, 0, False), (1, 0))
    block = kernel_rows(gram, norm_row, norm_lane, dim) - product_nt(pieces, pieces)
    inner = dot(centres, points_ref[...], (1, 1))
    base = high_ref[...], middle_ref[...], low_ref[...]
    resid = kernel_rows(inner, norm_row, norms_ref[...], dim) - product_nt(pieces, base)
    left = terms(share, 0, True)
    work_ref[:, :size] = block - dot(left, terms(share, 0, False), (0, 0))
    work_ref[:, size : 2 * size] = eye.astype(jnp.float32)
    work_ref[:, 128:] = resid - dot(left, terms(before, 0, False), (0, 0))
    upper = join(eliminate(tiles_of(work_ref, 0, size, 0, work_ref.shape[1] // 128), 0))
    cols = jnp.concatenate([before, upper[:, 128:]], axis=0)
    cols_ref[...] = cols.T
    diag_ref[...] = start_ref[...] - jnp.sum(cols * cols, axis=0, keepdims=True)


def exchange(chains, mesh):
    groups, devs = mesh.shape["group"], mesh.shape["dev"]

    def swap(value, partner):
        return lax.ppermute(value, AXES, [(i, partner(i)) for i in range(groups * devs)])

    def add(a, b):
        return a + b

    near = [1 << k for k in range(devs.bit_length() - 1)]
    far = [devs << k for k in range(1, groups.bit_length() - 1)]
    assert 1 << len(near) == devs and 2 << len(far) == groups
    steps = near[:1] + far + near[1:]
    turn = len(steps) // 2
    orders = (steps, steps[turn:] + steps[:turn])
    got = [swap(chains[2 * r + 1], lambda i: i ^ devs) for r in range(2)]
    sums = [add(chains[2 * r], got[r]) for r in range(2)]
    for k in range(len(steps)):
        got = [swap(sums[r], lambda i: i ^ orders[r][k]) for r in range(2)]
        sums = [add(sums[r], got[r]) for r in range(2)]
    k = len(steps) + 1
    got = [swap(sums[r], lambda i: i ^ devs) for r in range(2)]
    return sums[0], got[0], sums[1], got[1]


def vmem(n):
    return [pl.BlockSpec(memory_space=pltpu.VMEM)] * n


def per_device(points, base_factor, pivots, mesh):
    rows, dim = points.shape
    rounds, slots = pivots.shape
    base = base_factor.shape[1]
    piece = jax.ShapeDtypeStruct((slots // 2, dim + base), jnp.float32)
    n = 2 * rounds
    chains = pl.pallas_call(
        pick_kernel,
        out_shape=(piece,) * n
        + (jax.ShapeDtypeStruct(points.shape, points.dtype),)
        + (jax.ShapeDtypeStruct(base_factor.shape, jnp.bfloat16),) * 3
        + (jax.ShapeDtypeStruct((1, rows), jnp.float32),) * 2,
        in_specs=vmem(1) + [pl.BlockSpec(memory_space=pl.ANY)] * 2,
        out_specs=tuple(vmem(n + 6)),
        scratch_shapes=[pltpu.VMEM(base_factor.shape, base_factor.dtype), pltpu.SemaphoreType.DMA((2,))],
        compiler_params=pltpu.CompilerParams(vmem_limit_bytes=54380 * 1024),
        name="pick",
    )(pivots, points, base_factor)
    chains, local = chains[:n], chains[n:]
    parts = exchange(chains, mesh)
    width = dim + base
    half = jnp.bfloat16
    scratch = [pltpu.VMEM((slots, width), jnp.float32), pltpu.VMEM((slots, 128 + rows), jnp.float32)]
    *front, work = pl.pallas_call(
        zero_kernel,
        out_shape=(
            jax.ShapeDtypeStruct((slots, dim), half),
            jax.ShapeDtypeStruct((3 * slots, base), half),
            jax.ShapeDtypeStruct((slots, 128), jnp.float32),
            jax.ShapeDtypeStruct((slots, 128 + rows), jnp.float32),
        ),
        in_specs=vmem(7),
        out_specs=tuple(vmem(4)),
        scratch_shapes=scratch[:1],
        compiler_params=pltpu.CompilerParams(vmem_limit_bytes=16 * 2**20),
        cost_estimate=pl.CostEstimate(flops=10**7, bytes_accessed=2**19, transcendentals=0),
        name="blocks",
    )(*parts[:2], *local[:5])
    front += pl.pallas_call(
        first_kernel,
        out_shape=(jax.ShapeDtypeStruct((slots, 6 * slots), half), jax.ShapeDtypeStruct((slots, rows), jnp.float32)),
        in_specs=vmem(1),
        out_specs=tuple(vmem(2)),
        compiler_params=pltpu.CompilerParams(vmem_limit_bytes=16 * 2**20),
        cost_estimate=pl.CostEstimate(flops=10**7, bytes_accessed=2**19, transcendentals=0),
        name="first",
    )(work)
    cols, diag = pl.pallas_call(
        second_kernel,
        out_shape=(
            jax.ShapeDtypeStruct((rows, 2 * slots), jnp.float32),
            jax.ShapeDtypeStruct((1, rows), jnp.float32),
        ),
        in_specs=vmem(13),
        out_specs=tuple(vmem(2)),
        scratch_shapes=scratch,
        compiler_params=pltpu.CompilerParams(vmem_limit_bytes=16 * 2**20),
        name="second",
    )(*parts[2:], *local, *front)
    return cols, diag.reshape(rows)


def solution(mesh):
    return jax.shard_map(
        functools.partial(per_device, mesh=mesh),
        mesh=mesh,
        in_specs=(P(AXES, None), P(AXES, None), P()),
        out_specs=(P(AXES, None), P(AXES)),
        check_vma=False,
    )
```

```python
import functools

import jax
import jax.numpy as jnp
from jax import lax
from jax.experimental import pallas as pl
from jax.experimental.pallas import tpu as pltpu
from jax.sharding import PartitionSpec as P


AXES = ("group", "dev")


def pick_kernel(pivots_ref, points_hbm, base_hbm, *refs):
    outs, local, (base_ref, sems) = refs[:-6], refs[-6:-2], refs[-2:]
    points_ref, high_ref, middle_ref, low_ref = local
    copies = [pltpu.make_async_copy(points_hbm, points_ref, sems.at[0]), pltpu.make_async_copy(base_hbm, base_ref, sems.at[1])]
    for copy in copies:
        copy.start()
    rows, dim = points_ref.shape
    rounds, slots = pivots_ref.shape
    part = slots // 2
    device = lax.axis_index("group") * lax.axis_size("dev") + lax.axis_index("dev")
    first = lax.axis_index("group") % 2 == 0
    positions = lax.broadcasted_iota(jnp.int32, (rows, slots), 0) + device * rows
    chosen = [(positions == pivots_ref[r : r + 1, :]).astype(jnp.bfloat16) for r in range(rounds)]

    def put(lanes, pieces):
        for r in range(rounds):
            rows_of = sum(dot(chosen[r], piece, (0, 0)) for piece in pieces)
            outs[2 * r][:, lanes] = jnp.where(first, rows_of[:part], rows_of[part:])
            outs[2 * r + 1][:, lanes] = jnp.where(first, rows_of[part:], rows_of[:part])

    copies[0].wait()
    points = points_ref[...]
    put(slice(0, dim), (points,))
    copies[1].wait()
    base = base_ref[...]
    parts = split(base)
    put(slice(dim, None), parts)
    high_ref[...], middle_ref[...], low_ref[...] = parts


def dot(a, b, dims):
    return lax.dot_general(a, b, ((dims[:1], dims[1:]), ((), ())), preferred_element_type=jnp.float32)


def split(value):
    high = value.astype(jnp.bfloat16)
    rest = value - high.astype(jnp.float32)
    middle = rest.astype(jnp.bfloat16)
    low = (rest - middle.astype(jnp.float32)).astype(jnp.bfloat16)
    return high, middle, low


def product(a, b, dims):
    n = a[0].shape[0]
    first = dot(jnp.concatenate(a, axis=0), b[0], dims)
    second = dot(jnp.concatenate(a[:2], axis=0), b[1], dims)
    third = dot(a[0], b[2], dims)
    return first[:n] + (first[n : 2 * n] + second[:n]) + (first[2 * n :] + second[n:] + third)


def product_nt(a, b):
    return product(a, b, (1, 1))


def ahead(column):
    return 5 + column // 12


def spread(tile, sub):
    return jnp.broadcast_to(tile[sub:sub + 1, :], (8, 128))


def eliminate(panel, lane0):
    groups, tiles = len(panel), len(panel[0])
    b = 8 * groups
    row_id = lax.broadcasted_iota(jnp.int32, (8, 128), 0)

    def column(c):
        lane = lane0 + c
        return [jnp.broadcast_to(panel[g][0][:, lane : lane + 1], (8, 128)) if g >= c // 8 else None for g in range(groups)]

    rep = {}
    fresh = 0
    roots = [jnp.zeros((8, 128), jnp.float32) for _ in range(groups)]
    for j in range(b):
        while fresh < b and fresh - ahead(fresh) <= j:
            rep[fresh] = column(fresh)
            fresh += 1
        gj, sj = j // 8, j % 8
        mine = rep.pop(j)
        pivot = spread(mine[gj], sj)
        inverse = 1.0 / pivot
        roots[gj] = jnp.where(row_id == sj, lax.rsqrt(pivot), roots[gj])
        weight = [None if g < gj else mine[g] * inverse for g in range(groups)]
        weight[gj] = jnp.where(row_id > sj, weight[gj], 0.0)
        for c in sorted(rep):
            entry = spread(mine[c // 8], c % 8)
            for g in range(c // 8, groups):
                rep[c][g] = rep[c][g] - weight[g] * entry
        for t in range(tiles):
            line = spread(panel[gj][t], sj)
            for g in range(gj, groups):
                panel[g][t] = panel[g][t] - weight[g] * line
    return [[panel[g][t] * roots[g] for t in range(tiles)] for g in range(groups)]


def join(tiles):
    return jnp.concatenate([jnp.concatenate(row, axis=1) for row in tiles], axis=0)


def tiles_of(ref, row, count, tile0, tiles):
    return [[ref[row + 8 * g:row + 8 * g + 8, 128 * t:128 * t + 128] for t in range(tile0, tiles)] for g in range(count // 8)]


def kernel_rows(inner, row_norms, lane_norms, dim):
    return jnp.exp((-2.0 / dim) * (row_norms + lane_norms - 2.0 * inner))


def gather_rows(target, mine, other):
    part = mine.shape[0]
    core = lax.axis_index("group") % 2
    target[pl.ds(pl.multiple_of(core * part, part), part), :] = mine[...]
    target[pl.ds(pl.multiple_of((1 - core) * part, part), part), :] = other[...]


def zero_kernel(mine, other, points_ref, high_ref, middle_ref, low_ref, norms_ref, start_ref, centres_ref, pieces_ref, norm_ref, work_ref, rows_ref):
    gather_rows(rows_ref, mine, other)
    dim = points_ref.shape[1]
    size = rows_ref.shape[0]
    centres = rows_ref[:, :dim].astype(jnp.bfloat16)
    pieces = split(rows_ref[:, dim:])
    centres_ref[...] = centres
    pieces_ref[...] = jnp.concatenate(pieces, axis=0)
    gram = dot(centres, centres, (1, 1))
    eye = lax.broadcasted_iota(jnp.int32, (size, size), 0) == lax.broadcasted_iota(jnp.int32, (size, size), 1)
    own = jnp.where(eye, gram, 0.0)
    norm_lane = jnp.sum(own, axis=0, keepdims=True)
    norm_row = jnp.sum(own, axis=1, keepdims=True)
    norm_ref[...] = norm_lane
    work_ref[:, :size] = eye.astype(jnp.float32)
    work_ref[:, size : 2 * size] = kernel_rows(gram, norm_row, norm_lane, dim) - product_nt(pieces, pieces)
    points = points_ref[...]
    inner = dot(centres, points, (1, 1))
    base = high_ref[...], middle_ref[...], low_ref[...]
    ones = jnp.ones((8, dim), jnp.bfloat16)
    wide = points.astype(jnp.float32)
    norms = sum(dot(ones, x, (1, 1)) for x in split(wide * wide)[:2])[0:1, :]
    norms_ref[...] = norms
    whole = sum(x.astype(jnp.float32) for x in base)
    start_ref[...] = 1.0 - sum(dot(ones, x, (1, 1)) for x in split(whole * whole))[0:1, :]
    work_ref[:, 128:] = kernel_rows(inner, norm_row, norms, dim) - product_nt(pieces, base)


def first_kernel(work_ref, inverse_ref, cols_ref):
    size = work_ref.shape[0]
    upper = join(eliminate(tiles_of(work_ref, 0, size, 0, work_ref.shape[1] // 128), size))
    inverse_ref[...] = jnp.concatenate(split(upper[:, :size]), axis=0)
    cols_ref[...] = upper[:, 128:]


def second_kernel(mine, other, points_ref, high_ref, middle_ref, low_ref, norms_ref, start_ref, centres_ref, pieces_ref, norm_ref, inverse_ref, before_ref, cols_ref, diag_ref, rows_ref, work_ref):
    gather_rows(rows_ref, mine, other)
    dim = points_ref.shape[1]
    size = rows_ref.shape[0]
    centres = rows_ref[:, :dim].astype(jnp.bfloat16)
    pieces = split(rows_ref[:, dim:])
    before = before_ref[...]
    old = tuple(pieces_ref[k * size : (k + 1) * size, :] for k in range(3))
    inverse = tuple(inverse_ref[k * size : (k + 1) * size, :] for k in range(3))
    cross = dot(centres, centres_ref[...], (1, 1))
    gram = dot(centres, centres, (1, 1))
    eye = lax.broadcasted_iota(jnp.int32, (size, size), 0) == lax.broadcasted_iota(jnp.int32, (size, size), 1)
    own = jnp.where(eye, gram, 0.0)
    norm_lane = jnp.sum(own, axis=0, keepdims=True)
    norm_row = jnp.sum(own, axis=1, keepdims=True)
    cross = kernel_rows(cross, norm_row, norm_ref[...], dim) - product_nt(pieces, old)
    share = split(product_nt(split(cross), inverse))
    block = kernel_rows(gram, norm_row, norm_lane, dim) - product_nt(pieces, pieces)
    inner = dot(centres, points_ref[...], (1, 1))
    base = high_ref[...], middle_ref[...], low_ref[...]
    resid = kernel_rows(inner, norm_row, norms_ref[...], dim) - product_nt(pieces, base)
    work_ref[:, :size] = block - product_nt(share, share)
    work_ref[:, size : 2 * size] = eye.astype(jnp.float32)
    work_ref[:, 128:] = resid - product(share, split(before), (1, 0))
    upper = join(eliminate(tiles_of(work_ref, 0, size, 0, work_ref.shape[1] // 128), 0))
    cols = jnp.concatenate([before, upper[:, 128:]], axis=0)
    cols_ref[...] = cols.T
    diag_ref[...] = start_ref[...] - jnp.sum(cols * cols, axis=0, keepdims=True)


def exchange(chains, mesh):
    groups, devs = mesh.shape["group"], mesh.shape["dev"]

    def swap(value, partner):
        return lax.ppermute(value, AXES, [(i, partner(i)) for i in range(groups * devs)])

    def add(a, b):
        return a + b

    near = [1 << k for k in range(devs.bit_length() - 1)]
    far = [devs << k for k in range(1, groups.bit_length() - 1)]
    assert 1 << len(near) == devs and 2 << len(far) == groups
    steps = near[:1] + far + near[1:]
    turn = len(steps) // 2
    orders = (far + near, steps[turn:] + steps[:turn])
    got = [swap(chains[2 * r + 1], lambda i: i ^ devs) for r in range(2)]
    sums = [add(chains[2 * r], got[r]) for r in range(2)]
    for k in range(len(steps)):
        got = [swap(sums[r], lambda i: i ^ orders[r][k]) for r in range(2)]
        sums = [add(sums[r], got[r]) for r in range(2)]
    k = len(steps) + 1
    got = [swap(sums[r], lambda i: i ^ devs) for r in range(2)]
    return sums[0], got[0], sums[1], got[1]


def vmem(n):
    return [pl.BlockSpec(memory_space=pltpu.VMEM)] * n


def per_device(points, base_factor, pivots, mesh):
    rows, dim = points.shape
    rounds, slots = pivots.shape
    base = base_factor.shape[1]
    piece = jax.ShapeDtypeStruct((slots // 2, dim + base), jnp.float32)
    n = 2 * rounds
    chains = pl.pallas_call(
        pick_kernel,
        out_shape=(piece,) * n
        + (jax.ShapeDtypeStruct(points.shape, points.dtype),)
        + (jax.ShapeDtypeStruct(base_factor.shape, jnp.bfloat16),) * 3,
        in_specs=vmem(1) + [pl.BlockSpec(memory_space=pl.ANY)] * 2,
        out_specs=tuple(vmem(n + 4)),
        scratch_shapes=[pltpu.VMEM(base_factor.shape, base_factor.dtype), pltpu.SemaphoreType.DMA((2,))],
        compiler_params=pltpu.CompilerParams(vmem_limit_bytes=54380 * 1024),
        name="pick",
    )(pivots, points, base_factor)
    chains, local = chains[:n], chains[n:]
    parts = exchange(chains, mesh)
    width = dim + base
    half = jnp.bfloat16
    scratch = [pltpu.VMEM((slots, width), jnp.float32), pltpu.VMEM((slots, 128 + rows), jnp.float32)]
    norms, start, *front, work = pl.pallas_call(
        zero_kernel,
        out_shape=(
            jax.ShapeDtypeStruct((1, rows), jnp.float32),
            jax.ShapeDtypeStruct((1, rows), jnp.float32),
            jax.ShapeDtypeStruct((slots, dim), half),
            jax.ShapeDtypeStruct((3 * slots, base), half),
            jax.ShapeDtypeStruct((1, slots), jnp.float32),
            jax.ShapeDtypeStruct((slots, 128 + rows), jnp.float32),
        ),
        in_specs=vmem(6),
        out_specs=tuple(vmem(6)),
        scratch_shapes=scratch[:1],
        compiler_params=pltpu.CompilerParams(vmem_limit_bytes=16 * 2**20),
        cost_estimate=pl.CostEstimate(flops=10**7, bytes_accessed=2**19, transcendentals=0),
        name="blocks",
    )(*parts[:2], *local)
    front += pl.pallas_call(
        first_kernel,
        out_shape=(jax.ShapeDtypeStruct((3 * slots, slots), half), jax.ShapeDtypeStruct((slots, rows), jnp.float32)),
        in_specs=vmem(1),
        out_specs=tuple(vmem(2)),
        compiler_params=pltpu.CompilerParams(vmem_limit_bytes=16 * 2**20),
        cost_estimate=pl.CostEstimate(flops=10**7, bytes_accessed=2**19, transcendentals=0),
        name="first",
    )(work)
    cols, diag = pl.pallas_call(
        second_kernel,
        out_shape=(
            jax.ShapeDtypeStruct((rows, 2 * slots), jnp.float32),
            jax.ShapeDtypeStruct((1, rows), jnp.float32),
        ),
        in_specs=vmem(13),
        out_specs=tuple(vmem(2)),
        scratch_shapes=scratch,
        compiler_params=pltpu.CompilerParams(vmem_limit_bytes=16 * 2**20),
        name="second",
    )(*parts[2:], *local, norms, start, *front)
    return cols, diag.reshape(rows)


def solution(mesh):
    return jax.shard_map(
        functools.partial(per_device, mesh=mesh),
        mesh=mesh,
        in_specs=(P(AXES, None), P(AXES, None), P()),
        out_specs=(P(AXES, None), P(AXES)),
        check_vma=False,
    )
```
